32 devices in a mesh: prow: 4 (over y, x), pcol: 8 (over z, core).
Axes of the slice: x: 2, y: 2, z: 4, core: 2. Of those that a mesh axis runs over, the one named last changes fastest.
Arguments:
- inverse_factor: float32 [1024, 1024], P('pcol'), as said below
- diag_block: float32 [1024, 1024], P('pcol'), as said below
- panel_matrix: float32 [16, 4, 128, 1024], P(None, 'prow', 'pcol'), may hold values from -6 to 6
- panel_factor: float32 [16, 4, 128, 1024], P(None, 'prow', 'pcol'), may hold values from -0.1875 to 0.1875
- trailing: float32 [16, 4, 128, 8, 8, 128], P(None, 'prow', None, None, 'pcol'), may hold values from -6 to 6
Outputs:
- reduced_diag: float32 [1024, 1024], P('pcol')
- panel_result: float32 [16, 4, 128, 1024], P(None, 'prow', 'pcol')
- trailing_out: float32 [16, 4, 128, 8, 8, 128], P(None, 'prow', None, None, 'pcol')
The draws below stay inside these ranges and needn't reach their ends.
Inputs may be any that keep to these rules, and one draw needn't show every extreme that they name: `inverse_factor`: lower triangular, diagonal entries between 0.5 and 2. `diag_block`: symmetric.
All inputs are finite; a program needn't handle non-finite values.
Results may differ from the reference program's by a relative error of at most 0.0003.
Values sent between devices are 32-bit elements; how exact they have to be, the bound alone decides.
A program may use at most 128 MiB of HBM per device.

```python
import jax
import jax.numpy as jnp
from jax import lax

NB = 1024
TILE = 128
MR = 16
M = 8192
MC = 8
N_PROW = 4
N_PCOL = 8


def draw_inverse_factor(key, part):
    first, second = jax.random.split(jax.random.fold_in(key, 11), 2)
    spread = jax.random.normal(first, (NB, NB), jnp.float32) * (0.6 / NB ** 0.5)
    diagonal = jnp.exp(jax.random.uniform(second, (NB,), jnp.float32, -0.69, 0.69))
    return jnp.tril(spread, -1) + jnp.diag(diagonal)


def draw_diag_block(key, part):
    first = jax.random.fold_in(key, 23)
    base = jax.random.normal(first, (NB, NB), jnp.float32)
    return (base + base.T) * 0.70710678


def block_levels(stream_key, extent, cuts, low, largest):
    loudness = 1.0
    for axis_at, parts in cuts:
        steps = jax.random.uniform(jax.random.fold_in(jax.random.fold_in(stream_key, 6), axis_at), (parts,), jnp.float32, low / len(cuts), largest / len(cuts))
        loudness = loudness * jnp.repeat(jnp.exp(steps), extent[axis_at] // parts).reshape((-1,) + (1,) * (len(extent) - 1 - axis_at))
    return loudness


def centred(stream_key, extent, scale, most, pieces=(), held_as=jnp.bfloat16):
    entries = scale * jax.random.normal(stream_key, extent, jnp.float32)
    if pieces:
        entries = entries * block_levels(stream_key, extent, pieces, -0.22, 0.18)
    return jnp.clip(entries, -most, most).astype(held_as)


def setup_inputs(seed: int = 0) -> dict:
    keys = jax.random.split(jax.random.key(seed), 6)
    return {
        "inverse_factor": draw_inverse_factor(jax.random.fold_in(keys[5], 71), 0),
        "diag_block": draw_diag_block(jax.random.fold_in(keys[5], 71), 0),
        "panel_matrix": centred(keys[2], (MR, N_PROW, TILE, NB), 1.0, 6.0, ((1, 4), (2, 8)), jnp.float32),
        "panel_factor": centred(keys[3], (MR, N_PROW, TILE, NB), NB ** -0.5, 0.1875, ((1, 4), (2, 8)), jnp.float32),
        "trailing": centred(keys[4], (MR, N_PROW, TILE, MC, N_PCOL, TILE), 1.0, 6.0, ((1, 4), (4, 8)), jnp.float32),
    }


def reference(inverse_factor, diag_block, panel_matrix, panel_factor, trailing):
    exact = lax.Precision.HIGHEST
    order = M
    inner = jnp.dot(diag_block, inverse_factor.T, precision=exact, preferred_element_type=jnp.float32)
    reduced = jnp.dot(inverse_factor, inner, precision=exact, preferred_element_type=jnp.float32)
    panel = panel_matrix.reshape(order, NB)
    factor = panel_factor.reshape(order, NB)
    solved = jnp.dot(panel, inverse_factor.T, precision=exact, preferred_element_type=jnp.float32)
    coupled = jnp.dot(factor, reduced, precision=exact, preferred_element_type=jnp.float32)
    shifted = solved - 0.5 * coupled
    result = shifted - 0.5 * coupled
    whole = trailing.reshape(order, order)
    col_tile = jnp.arange(order, dtype=jnp.int32) // TILE

    def one_row(index):
        start = (index * TILE).astype(jnp.int32)
        rows_a = lax.dynamic_slice_in_dim(whole, start, TILE, 0)
        rows_y = lax.dynamic_slice_in_dim(shifted, start, TILE, 0)
        rows_f = lax.dynamic_slice_in_dim(factor, start, TILE, 0)
        update = jnp.dot(rows_y, factor.T, precision=exact, preferred_element_type=jnp.float32)
        update = update + jnp.dot(rows_f, shifted.T, precision=exact, preferred_element_type=jnp.float32)
        return jnp.where(col_tile[None, :] <= index, rows_a - update, rows_a)

    blocks = lax.map(one_row, jnp.arange(order // TILE, dtype=jnp.int32))
    trailing_out = blocks.reshape(trailing.shape)
    return reduced, result.reshape(panel_matrix.shape), trailing_out
```

```python
import functools

import jax
import jax.numpy as jnp
from jax import lax
from jax.experimental import pallas as pl
from jax.experimental.pallas import tpu as pltpu
from jax.sharding import PartitionSpec as P

AXES = ("prow", "pcol")
WHOLE_LIMIT = 40 * 2**20


def split(x):
    high = x.astype(jnp.bfloat16)
    low = (x - high.astype(jnp.float32)).astype(jnp.bfloat16)
    return high, low


def dot(a, b):
    return jnp.dot(a, b, precision=lax.Precision.HIGH, preferred_element_type=jnp.float32)


def mul_t(a, b):
    return lax.dot_general(a, b, (((1,), (1,)), ((), ())), preferred_element_type=jnp.float32)


def update_kernel(
    grid_rows, grid_cols, group, wide, ids,
    rows_y, rows_f, cols_y, cols_f, old, new,
    ry_h, ry_l, rf_h, rf_l, cy_h, cy_l, cf_h, cf_l,
):
    step = pl.program_id(0)
    col_tiles = cols_y.shape[2]
    tile = old.shape[1]

    @pl.when(step == 0)
    def _():
        for source, high, low in ((cols_y, cy_h, cy_l), (cols_f, cf_h, cf_l)):
            @pl.loop(0, col_tiles)
            def _(j):
                h, l = split(source[0, :, j, 0].reshape(tile, -1))
                at = pl.ds(pl.multiple_of(j * tile, tile), tile)
                high[at, :] = h
                low[at, :] = l

    for source, high, low in ((rows_y, ry_h, ry_l), (rows_f, rf_h, rf_l)):
        @pl.loop(0, group)
        def _(i):
            h, l = split(source[0, :, i].reshape(tile, -1))
            at = pl.ds(pl.multiple_of(i * tile, tile), tile)
            high[at, :] = h
            low[at, :] = l
    new[...] = old[...]
    span = wide * tile
    last = (step * group + group - 1) * grid_rows + grid_rows - 1
    count = lax.min(last // (grid_cols * wide) + 1, col_tiles // wide)

    for b in range(col_tiles // wide):
        @pl.when(b < count)
        def _():
            at = pl.ds(b * span, span)
            fh, yh = cf_h[at, :], cy_h[at, :]
            total = mul_t(ry_h[...], fh) + mul_t(ry_l[...], fh) + mul_t(ry_h[...], cf_l[at, :])
            total += mul_t(rf_h[...], yh) + mul_t(rf_l[...], yh) + mul_t(rf_h[...], cy_l[at, :])
            for i in range(group):
                row = (step * group + i) * grid_rows + ids[0]
                for w in range(wide):
                    j = b * wide + w
                    @pl.when(row >= j * grid_cols + ids[1])
                    def _():
                        part = total[i * tile:(i + 1) * tile, w * tile:(w + 1) * tile]
                        new[i, :, j, :] = old[i, :, j, :] - part


def spread(x, tile_rows, col_tiles):
    grid_rows, grid_cols = lax.axis_size("prow"), lax.axis_size("pcol")
    column, row = lax.axis_index("pcol"), lax.axis_index("prow")
    stride = grid_cols // grid_rows
    piece, width = x.shape[0] // tile_rows, x.shape[1]
    root, picked = column % grid_rows, column // grid_rows
    by_row = (-1, grid_cols, tile_rows, piece, width)
    by_col = (-1, grid_cols, col_tiles, stride, piece, width)
    if x.size * 4 * grid_rows * grid_cols <= WHOLE_LIMIT:
        everything = lax.all_gather(x, AXES, axis=0, tiled=False)
        return everything.reshape(by_row), everything.reshape(by_col), (row, root, picked)
    rows = lax.all_gather(x, "pcol", axis=0, tiled=False)
    cols = lax.dynamic_index_in_dim(rows.reshape(by_col), picked, 3, keepdims=True)
    cols = lax.psum(jnp.where(row == root, cols, jnp.zeros_like(cols)), "prow")
    return rows.reshape(by_row), cols, (0, 0, 0)


def update(y_parts, f_parts, trailing):
    grid_rows, grid_cols = lax.axis_size("prow"), lax.axis_size("pcol")
    tile_rows, tile, col_tiles = trailing.shape[0], trailing.shape[2], trailing.shape[3]
    y_rows, y_cols, places = y_parts
    f_rows, f_cols, _ = f_parts
    piece, width = y_rows.shape[-2:]
    column, row = lax.axis_index("pcol"), lax.axis_index("prow")
    ids = jnp.stack([jnp.int32(v) for v in (row, column) + places])
    group = 4 if tile_rows % 4 == 0 else 1
    wide = 2 if col_tiles % 2 == 0 else 1
    rows = pl.BlockSpec((1, grid_cols, group, piece, width), lambda s, d: (d[2], 0, s, 0, 0))
    cols = pl.BlockSpec(
        (1, grid_cols, col_tiles, 1, piece, width), lambda s, d: (d[3], 0, 0, d[4], 0, 0),
        pipeline_mode=pl.Buffered(1),
    )
    block = pl.BlockSpec((group, tile, col_tiles, tile), lambda s, d: (s, 0, 0, 0))
    row_scratch = pltpu.VMEM((group * tile, width), jnp.bfloat16)
    col_scratch = pltpu.VMEM((col_tiles * tile, width), jnp.bfloat16)
    old = trailing.reshape(tile_rows, tile, col_tiles, tile)
    new = pl.pallas_call(
        functools.partial(update_kernel, grid_rows, grid_cols, group, wide),
        out_shape=jax.ShapeDtypeStruct(old.shape, jnp.float32),
        grid_spec=pltpu.PrefetchScalarGridSpec(
            num_scalar_prefetch=1, grid=(tile_rows // group,),
            in_specs=[rows, rows, cols, cols, block], out_specs=block,
            scratch_shapes=[row_scratch] * 4 + [col_scratch] * 4,
        ),
        compiler_params=pltpu.CompilerParams(vmem_limit_bytes=60 * 2**20),
    )(
        ids, y_rows, f_rows, y_cols, f_cols, old,
    )
    return new.reshape(trailing.shape)


def body(inverse_factor, diag_block, panel_matrix, panel_factor, trailing):
    grid_rows, grid_cols = lax.axis_size("prow"), lax.axis_size("pcol")
    row = lax.axis_index("prow")
    local, width = inverse_factor.shape
    share = local // grid_rows
    both = jnp.stack([
        lax.dynamic_slice_in_dim(inverse_factor, row * share, share, 0),
        lax.dynamic_slice_in_dim(diag_block, row * share, share, 0),
    ])
    both = lax.all_gather(both, AXES, axis=0, tiled=False)
    both = both.reshape(grid_rows, grid_cols, 2, share, width).transpose(2, 1, 0, 3, 4)
    inverse, diag = both.reshape(2, grid_cols * local, width)
    factor = panel_factor.reshape(-1, width)
    sizes = trailing.shape[0], trailing.shape[3]
    f_parts = spread(factor, *sizes)
    panel = panel_matrix.reshape(-1, width)
    mid = dot(dot(factor, inverse), diag)
    shifted = dot(panel - 0.5 * mid, inverse.T)
    y_parts = spread(shifted, *sizes)
    panel_result = dot(panel - mid, inverse.T).reshape(panel_matrix.shape)
    reduced = dot(dot(inverse_factor, diag), inverse.T)
    return reduced, panel_result, update(y_parts, f_parts, trailing)


def solution(mesh):
    in_specs = (
        P("pcol", None),
        P("pcol", None),
        P(None, "prow", "pcol", None),
        P(None, "prow", "pcol", None),
        P(None, "prow", None, None, "pcol", None),
    )
    out_specs = (
        P("pcol", None),
        P(None, "prow", "pcol", None),
        P(None, "prow", None, None, "pcol", None),
    )
    return jax.shard_map(body, mesh=mesh, in_specs=in_specs, out_specs=out_specs, check_vma=False)
```

```python
import functools

import jax
import jax.numpy as jnp
from jax import lax
from jax.experimental import pallas as pl
from jax.experimental.pallas import tpu as pltpu
from jax.sharding import PartitionSpec as P

AXES = ("prow", "pcol")


def split(x):
    high = x.astype(jnp.bfloat16)
    low = (x - high.astype(jnp.float32)).astype(jnp.bfloat16)
    return high, low


def dot(a, b):
    return jnp.dot(a, b, precision=lax.Precision.HIGH, preferred_element_type=jnp.float32)


def mul_t(a, b):
    return lax.dot_general(a, b, (((1,), (1,)), ((), ())), preferred_element_type=jnp.float32)


def update_kernel(
    grid_rows, grid_cols, group, wide, ids,
    rows_y, rows_f, cols_y, cols_f, old, new,
    ry_h, ry_l, rf_h, rf_l, cy_h, cy_l, cf_h, cf_l,
):
    step = pl.program_id(0)
    col_tiles = cols_y.shape[2]
    tile = old.shape[1]

    @pl.when(step == 0)
    def _():
        for source, high, low in ((cols_y, cy_h, cy_l), (cols_f, cf_h, cf_l)):
            @pl.loop(0, col_tiles)
            def _(j):
                h, l = split(source[0, :, j, 0].reshape(tile, -1))
                at = pl.ds(pl.multiple_of(j * tile, tile), tile)
                high[at, :] = h
                low[at, :] = l

    for source, high, low in ((rows_y, ry_h, ry_l), (rows_f, rf_h, rf_l)):
        @pl.loop(0, group)
        def _(i):
            h, l = split(source[0, :, i].reshape(tile, -1))
            at = pl.ds(pl.multiple_of(i * tile, tile), tile)
            high[at, :] = h
            low[at, :] = l
    new[...] = old[...]
    span = wide * tile
    last = (step * group + group - 1) * grid_rows + grid_rows - 1
    count = lax.min(last // (grid_cols * wide) + 1, col_tiles // wide)

    for b in range(col_tiles // wide):
        @pl.when(b < count)
        def _():
            at = pl.ds(b * span, span)
            fh, yh = cf_h[at, :], cy_h[at, :]
            total = mul_t(ry_h[...], fh) + mul_t(ry_l[...], fh) + mul_t(ry_h[...], cf_l[at, :])
            total += mul_t(rf_h[...], yh) + mul_t(rf_l[...], yh) + mul_t(rf_h[...], cy_l[at, :])
            for i in range(group):
                row = (step * group + i) * grid_rows + ids[0]
                for w in range(wide):
                    j = b * wide + w
                    @pl.when(row >= j * grid_cols + ids[1])
                    def _():
                        part = total[i * tile:(i + 1) * tile, w * tile:(w + 1) * tile]
                        new[i, :, j, :] = old[i, :, j, :] - part


def spread(x, tile_rows, col_tiles):
    grid_rows, grid_cols = lax.axis_size("prow"), lax.axis_size("pcol")
    column, row = lax.axis_index("pcol"), lax.axis_index("prow")
    stride = grid_cols // grid_rows
    piece, width = x.shape[0] // tile_rows, x.shape[1]
    root, picked = column % grid_rows, column // grid_rows
    by_row = (-1, grid_cols, tile_rows, piece, width)
    by_col = (-1, grid_cols, col_tiles, stride, piece, width)
    rows = lax.all_gather(x, "pcol", axis=0, tiled=False)
    own = lax.dynamic_index_in_dim(rows.reshape(by_col), picked, 3, keepdims=True)
    cols = jnp.where(row == root, own, jnp.zeros_like(own))
    for k in range(1, grid_rows):
        pairs = [
            ((c % grid_rows) * grid_cols + c, ((c % grid_rows + k) % grid_rows) * grid_cols + c)
            for c in range(grid_cols)
        ]
        cols = cols + lax.ppermute(own, AXES, pairs)
    return rows.reshape(by_row), cols, (0, 0, 0)


def update(y_parts, f_parts, trailing):
    grid_rows, grid_cols = lax.axis_size("prow"), lax.axis_size("pcol")
    tile_rows, tile, col_tiles = trailing.shape[0], trailing.shape[2], trailing.shape[3]
    y_rows, y_cols, places = y_parts
    f_rows, f_cols, _ = f_parts
    piece, width = y_rows.shape[-2:]
    column, row = lax.axis_index("pcol"), lax.axis_index("prow")
    ids = jnp.stack([jnp.int32(v) for v in (row, column) + places])
    group = 4 if tile_rows % 4 == 0 else 1
    wide = 2 if col_tiles % 2 == 0 else 1
    rows = pl.BlockSpec((1, grid_cols, group, piece, width), lambda s, d: (d[2], 0, s, 0, 0))
    cols = pl.BlockSpec(
        (1, grid_cols, col_tiles, 1, piece, width), lambda s, d: (d[3], 0, 0, d[4], 0, 0),
        pipeline_mode=pl.Buffered(1),
    )
    block = pl.BlockSpec((group, tile, col_tiles, tile), lambda s, d: (s, 0, 0, 0))
    row_scratch = pltpu.VMEM((group * tile, width), jnp.bfloat16)
    col_scratch = pltpu.VMEM((col_tiles * tile, width), jnp.bfloat16)
    old = trailing.reshape(tile_rows, tile, col_tiles, tile)
    new = pl.pallas_call(
        functools.partial(update_kernel, grid_rows, grid_cols, group, wide),
        out_shape=jax.ShapeDtypeStruct(old.shape, jnp.float32),
        grid_spec=pltpu.PrefetchScalarGridSpec(
            num_scalar_prefetch=1, grid=(tile_rows // group,),
            in_specs=[rows, rows, cols, cols, block], out_specs=block,
            scratch_shapes=[row_scratch] * 4 + [col_scratch] * 4,
        ),
        compiler_params=pltpu.CompilerParams(vmem_limit_bytes=60 * 2**20),
    )(
        ids, y_rows, f_rows, y_cols, f_cols, old,
    )
    return new.reshape(trailing.shape)


def body(inverse_factor, diag_block, panel_matrix, panel_factor, trailing):
    grid_rows, grid_cols = lax.axis_size("prow"), lax.axis_size("pcol")
    row = lax.axis_index("prow")
    local, width = inverse_factor.shape
    share = local // grid_rows
    both = jnp.stack([
        lax.dynamic_slice_in_dim(inverse_factor, row * share, share, 0),
        lax.dynamic_slice_in_dim(diag_block, row * share, share, 0),
    ])
    both = lax.all_gather(both, AXES, axis=0, tiled=False)
    both = both.reshape(grid_rows, grid_cols, 2, share, width).transpose(2, 1, 0, 3, 4)
    inverse, diag = both.reshape(2, grid_cols * local, width)
    factor = panel_factor.reshape(-1, width)
    sizes = trailing.shape[0], trailing.shape[3]
    f_parts = spread(factor, *sizes)
    panel = panel_matrix.reshape(-1, width)
    mid = dot(dot(factor, inverse), diag)
    shifted = dot(panel - 0.5 * mid, inverse.T)
    y_parts = spread(shifted, *sizes)
    panel_result = dot(panel - mid, inverse.T).reshape(panel_matrix.shape)
    reduced = dot(dot(inverse_factor, diag), inverse.T)
    return reduced, panel_result, update(y_parts, f_parts, trailing)


def solution(mesh):
    in_specs = (
        P("pcol", None),
        P("pcol", None),
        P(None, "prow", "pcol", None),
        P(None, "prow", "pcol", None),
        P(None, "prow", None, None, "pcol", None),
    )
    out_specs = (
        P("pcol", None),
        P(None, "prow", "pcol", None),
        P(None, "prow", None, None, "pcol", None),
    )
    return jax.shard_map(body, mesh=mesh, in_specs=in_specs, out_specs=out_specs, check_vma=False)
```
